32 devices in a mesh: dp: 4 (over y, x), expert: 8 (over z, core).
Axes of the slice: x: 2, y: 2, z: 4, core: 2. Of those that a mesh axis runs over, the one named last changes fastest.
Arguments:
- hidden: bfloat16 [49152, 1024], P(('dp', 'expert')), may hold values from -6 to 6
- dout: bfloat16 [49152, 7168], P(('dp', 'expert')), may hold values from -1536 to 1536
- counts: int32 [32, 256], P(('dp', 'expert')), may hold values from 1 to 1536, as said below
- bucket_expert: int32 [1], replicated, may hold values from 0 to 255
- param: float32 [1024, 7168], P(('dp', 'expert')), may hold values from -0.1875 to 0.1875
- momentum: float32 [1024, 7168], P(('dp', 'expert')), may hold values from -3 to 3
Outputs:
- new_param: float32 [1024, 7168], P(('dp', 'expert'))
- new_momentum: float32 [1024, 7168], P(('dp', 'expert'))
- direction: float32 [1024, 7168], P(('dp', 'expert'))
The draws below stay inside these ranges and needn't reach their ends.
Inputs may be any that keep to these rules, and one draw needn't show every extreme that they name: `counts`: row k is device k's count; its rows k * 1536 + t with t below the count are live. For every expert some device has exactly 1536.
All inputs are finite; a program needn't handle non-finite values.
Results may differ from the reference program's by a relative error of at most 0.0003.
Values sent between devices are 32-bit elements; how exact they have to be, the bound alone decides.
A program may use at most 128 MiB of HBM per device.

```python
import jax
import jax.numpy as jnp
from jax import lax

FW = 1024
DW = 7168
NE = 256
TOK_DEV = 1536
TOKENS = 49152
N_DP = 4
N_EXPERT = 8


def draw_counts(key, part):
    ndevices = N_DP * N_EXPERT
    first_key, second_key = jax.random.split(jax.random.fold_in(key, 17))
    device = lax.broadcasted_iota(jnp.int32, (ndevices, NE), 0)
    ceiling = TOK_DEV * (ndevices + 2 * device) // (3 * ndevices)
    drawn = jax.random.randint(first_key, (ndevices, NE), 0, 1 << 20) % (ceiling + 1)
    drawn = jnp.maximum(drawn, 1)
    busiest = jax.random.randint(second_key, (1, NE), 0, ndevices)
    return jnp.where(device == busiest, TOK_DEV, drawn).astype(jnp.int32)


def with_spikes(values, key, source, target, blocks, factor):
    owner, partner = [(jnp.arange(values.shape[dim]) // (values.shape[dim] // blocks)).reshape([-1 if axis == dim else 1 for axis in range(values.ndim)]) for dim in (source, target)]
    chosen = jax.random.permutation(key, blocks)[partner]
    strong = (owner == chosen) | (owner == (partner + blocks // 2) % blocks)
    return jnp.where(strong, factor * values, values)


def block_levels(own_key, dims, shards, low, high):
    def one(dim, shards_of):
        heights = jax.random.uniform(jax.random.fold_in(jax.random.fold_in(own_key, 6), dim), (shards_of,), jnp.float32, low / len(shards), high / len(shards))
        return jnp.repeat(jnp.exp(heights), dims[dim] // shards_of).reshape((-1,) + (1,) * (len(dims) - dim - 1))

    level = one(*shards[0])
    for cut in shards[1:]:
        level = level * one(*cut)
    return level


def gaussian(key, extent, spread, most, shards=(), held_as=jnp.bfloat16):
    loudness = block_levels(key, extent, shards, -0.22, 0.18) if shards else 1.0
    values = jax.random.normal(key, extent, jnp.float32) * spread * loudness
    return jnp.minimum(jnp.maximum(values, -most), most).astype(held_as)


def bell_draw_with(own_key, shape, width, most, cuts, heavy, kind=jnp.bfloat16):
    entries = width * jax.random.normal(own_key, shape, jnp.float32)
    if cuts:
        entries = entries * block_levels(own_key, shape, cuts, -0.22, 0.18)
    return jnp.clip(with_spikes(entries, jax.random.fold_in(own_key, 3), *heavy), -most, most).astype(kind)


def setup_inputs(seed: int = 0) -> dict:
    arg_keys = jax.random.split(jax.random.key(seed), 7)
    hidden = bell_draw_with(arg_keys[0], (TOKENS, FW), 1.0, 6.0, ((0, 32),), (0, 1, 32, 2.75))
    dout = gaussian(arg_keys[1], (TOKENS, DW), (TOK_DEV // 6), 1536.0, ((0, 32),))
    counts = draw_counts(jax.random.fold_in(arg_keys[6], 71), 0)
    bucket_expert = jax.random.randint(arg_keys[3], (1,), 0, NE).astype(jnp.int32)
    param = gaussian(arg_keys[4], (FW, DW), FW ** -0.5, 0.1875, ((0, 32),), jnp.float32)
    momentum = gaussian(arg_keys[5], (FW, DW), 0.5, 3.0, ((0, 32),), jnp.float32)
    return dict(hidden=hidden, dout=dout, counts=counts, bucket_expert=bucket_expert, param=param, momentum=momentum)


first_beta = 0.9
second_beta = 0.99
decay_rate = 0.1
learn_rate = 0.001
soft_width = 0.05


def reference(hidden, dout, counts, bucket_expert, param, momentum):
    catalog = jnp.arange(counts.shape[1], dtype=jnp.int32)[None, :]
    local = jnp.sum(jnp.where(catalog == bucket_expert[0], counts, 0), axis=1).astype(jnp.int32)
    total = jnp.sum(local).astype(jnp.float32)
    position = jnp.arange(hidden.shape[0], dtype=jnp.int32) % TOK_DEV
    limit = jnp.repeat(local, TOK_DEV, total_repeat_length=hidden.shape[0])
    masked = jnp.where((position < limit)[:, None], hidden, jnp.zeros_like(hidden))
    summed = lax.dot_general(masked, dout, (((0,), (0,)), ((), ())), preferred_element_type=jnp.float32)
    grad = summed / total
    blend = first_beta * momentum + (1.0 - first_beta) * grad
    direction = jnp.tanh(blend / soft_width) + decay_rate * param
    new_param = param - learn_rate * direction
    new_momentum = second_beta * momentum + (1.0 - second_beta) * grad
    return new_param, new_momentum, direction
```

```python
import functools

import jax
import jax.numpy as jnp
from jax import lax
from jax.experimental import pallas as pl
from jax.experimental.pallas import tpu as pltpu
from jax.sharding import PartitionSpec as P

first_beta = 0.9
second_beta = 0.99
decay_rate = 0.1
learn_rate = 0.001
soft_width = 0.05

WIDTH = 256
LAGS = (2, 8, 13, 16, 19)
SLOTS = 3
HELD = LAGS[-1] + 1
MESH = pl.DeviceIdType.MESH


def block_product(columns, dout):
    dims = (((0,), (0,)), ((), ()))
    return lax.dot_general(columns, dout, dims, preferred_element_type=jnp.float32)


def mask_tokens(hidden, counts, bucket_expert):
    catalog = lax.broadcasted_iota(jnp.int32, counts.shape, 1)
    own_count = jnp.sum(jnp.where(catalog == bucket_expert[0], counts, 0))
    position = lax.broadcasted_iota(jnp.int32, (hidden.shape[0], 1), 0)
    return own_count, jnp.where(position < own_count, hidden, jnp.zeros_like(hidden))


def lion(grad, param, momentum):
    blend = first_beta * momentum + (1.0 - first_beta) * grad
    direction = jnp.tanh(blend / soft_width) + decay_rate * param
    new_param = param - learn_rate * direction
    new_momentum = second_beta * momentum + (1.0 - second_beta) * grad
    return (new_param, new_momentum, direction)


def plain_body(hidden, dout, counts, bucket_expert, param, momentum):
    own_count, masked = mask_tokens(hidden, counts, bucket_expert)
    total = lax.psum(own_count, ("dp", "expert")).astype(jnp.float32)
    shard = lax.psum_scatter(
        block_product(masked, dout), ("dp", "expert"), scatter_dimension=0, tiled=True
    )
    return lion(shard / total, param, momentum)


def reduce_kernel(
    chunks, ht_ref, dout_ref, count_ref, shard_ref, total_ref,
    acc, r0, r1, r2, r3, r4, tiles, count_in,
    tile_sem, send_sem, recv_sem, count_send, count_recv,
):
    rows = acc.shape[2]
    landing = (r0, r1, r2, r3, r4)
    dp = lax.axis_index("dp")
    ex = lax.axis_index("expert")
    y, x = lax.div(dp, 2), lax.rem(dp, 2)
    z1, z0, core = lax.div(ex, 4), lax.rem(lax.div(ex, 2), 2), lax.rem(ex, 2)
    step_x, step_y = 1 - 2 * x, 2 - 4 * y
    step_core, step_z0, step_z1 = 1 - 2 * core, 2 - 4 * z0, 4 - 8 * z1
    partners = (
        (dp, ex + step_core), (dp + step_x, ex), (dp + step_y, ex),
        (dp, ex + step_z0), (dp, ex + step_z1),
    )

    def tile_copy(c):
        slot = lax.rem(c, SLOTS)
        columns = pl.ds(pl.multiple_of(c * WIDTH, WIDTH), WIDTH)
        return pltpu.make_async_copy(
            dout_ref.at[:, columns], tiles.at[slot], tile_sem.at[slot]
        )

    def kind(c):
        z_first = lax.div(lax.rem(c, 4), 2) * (1 - lax.div(lax.div(c, 12) + 1, 2))
        return z_first, lax.rem(c, 2)

    def exchange(c, stage):
        half = landing[stage].shape[1]
        if stage == 0:
            target = (dp, ex + step_core)
        else:
            z_first, parity = kind(c)
            on_dp = z_first if stage >= 3 else 1 - z_first
            swap = parity if stage in (1, 3) else 1 - parity
            step_dp = (1 - swap) * step_x + swap * step_y
            step_ex = step_z0 if stage in (1, 3) else step_z1
            target = (dp + on_dp * step_dp, ex + (1 - on_dp) * step_ex)
        return pltpu.make_async_remote_copy(
            src_ref=acc.at[lax.rem(c, HELD), pl.ds(half, half)],
            dst_ref=landing[stage].at[c],
            send_sem=send_sem.at[stage, c],
            recv_sem=recv_sem.at[stage, c],
            device_id=target,
            device_id_type=MESH,
        )

    def count_exchange(stage):
        return pltpu.make_async_remote_copy(
            src_ref=count_in.at[stage],
            dst_ref=count_in.at[5 + stage],
            send_sem=count_send.at[stage],
            recv_sem=count_recv.at[stage],
            device_id=partners[stage],
            device_id_type=MESH,
        )

    for c in range(SLOTS):
        tile_copy(c).start()
    barrier = pltpu.get_barrier_semaphore()
    for partner in partners:
        pl.semaphore_signal(barrier, inc=1, device_id=partner, device_id_type=MESH)
    pl.semaphore_wait(barrier, 5)
    count_in[0] = count_ref[...]
    count_exchange(0).start()

    def multiply(c):
        tile_copy(c).wait()
        z_first, parity = kind(c)
        w_first, w_second = 8 - 6 * z_first, 4 - 3 * z_first
        w_x = (1 - parity) * w_first + parity * w_second
        w_y = parity * w_first + (1 - parity) * w_second
        w_z0, w_z1 = 2 + 6 * z_first, 1 + 3 * z_first
        mine = (y, x, z1, z0, core)
        weights = (w_y, w_x, w_z1, w_z0, 16)
        off = [
            [bit * weight for bit, weight in zip(mine, weights)],
            [(1 - bit) * weight for bit, weight in zip(mine, weights)],
        ]
        product = jnp.dot(
            ht_ref[...], tiles[lax.rem(c, SLOTS)], preferred_element_type=jnp.float32
        )
        held = lax.rem(c, HELD)
        for block in range(2 ** len(mine)):
            place = 0
            for i in range(len(mine)):
                place = place + off[(block >> (len(mine) - 1 - i)) & 1][i]
            acc[held, place] = product[block * rows:(block + 1) * rows]
        exchange(c, 0).start()

        @pl.when(c + SLOTS < chunks)
        def _():
            tile_copy(c + SLOTS).start()

    def fold(c, stage):
        half = landing[stage].shape[1]
        exchange(c, stage).wait_recv()
        held = lax.rem(c, HELD)
        acc[held, 0:half] = acc[held, 0:half] + landing[stage][c]
        exchange(c, stage + 1).start()

    def finish(c):
        exchange(c, 4).wait_recv()
        columns = pl.ds(pl.multiple_of(c * WIDTH, WIDTH), WIDTH)
        shard_ref[:, columns] = acc[lax.rem(c, HELD), 0] + r4[c, 0]
        for stage in range(5):
            exchange(c, stage).wait_send()

    def step(k, carry):
        @pl.when(k < chunks)
        def _():
            multiply(k)

        for stage in range(4):
            c = k - LAGS[stage]

            @pl.when((c >= 0) & (c < chunks))
            def _():
                fold(c, stage)

        c = k - LAGS[4]

        @pl.when(c >= 0)
        def _():
            finish(c)

        for stage in range(4):
            @pl.when(k == 3 * stage + 3)
            def _():
                count_exchange(stage).wait_recv()
                count_in[stage + 1] = count_in[stage] + count_in[5 + stage]
                count_exchange(stage + 1).start()

        return carry

    lax.fori_loop(0, chunks + LAGS[4], step, 0)
    count_exchange(4).wait_recv()
    total_ref[...] = count_in[4] + count_in[9]

    for stage in range(5):
        count_exchange(stage).wait_send()


def fast_body(devices, hidden, dout, counts, bucket_expert, param, momentum):
    own_count, masked = mask_tokens(hidden, counts, bucket_expert)
    tokens, features = hidden.shape
    width = dout.shape[1]
    rows = features // devices
    chunks = width // WIDTH
    spread = jnp.full((8, 128), own_count.astype(jnp.float32))
    vmem = pl.BlockSpec(memory_space=pltpu.VMEM)
    shard, total = pl.pallas_call(
        functools.partial(reduce_kernel, chunks),
        out_shape=(
            jax.ShapeDtypeStruct((rows, width), jnp.float32),
            jax.ShapeDtypeStruct((8, 128), jnp.float32),
        ),
        in_specs=[vmem, pl.BlockSpec(memory_space=pl.ANY), vmem],
        out_specs=(vmem, vmem),
        scratch_shapes=[pltpu.VMEM((HELD, devices, rows, WIDTH), jnp.float32)]
        + [
            pltpu.VMEM((chunks, devices >> (s + 1), rows, WIDTH), jnp.float32)
            for s in range(5)
        ]
        + [
            pltpu.VMEM((SLOTS, tokens, WIDTH), jnp.bfloat16),
            pltpu.VMEM((10, 8, 128), jnp.float32),
            pltpu.SemaphoreType.DMA((SLOTS,)),
            pltpu.SemaphoreType.DMA((5, chunks)),
            pltpu.SemaphoreType.DMA((5, chunks)),
            pltpu.SemaphoreType.DMA((5,)),
            pltpu.SemaphoreType.DMA((5,)),
        ],
        compiler_params=pltpu.CompilerParams(
            collective_id=0, has_side_effects=True, vmem_limit_bytes=67043328
        ),
    )(masked.T, dout, spread)
    return lion(shard / total[0, 0], param, momentum)


def solution(mesh):
    spec = P(("dp", "expert"), None)
    in_specs = (spec, spec, spec, P(), spec, spec)
    out_specs = (spec, spec, spec)
    if mesh.shape["dp"] == 4 and mesh.shape["expert"] == 8:
        body = functools.partial(fast_body, mesh.size)
    else:
        body = plain_body
    return jax.shard_map(body, mesh=mesh, in_specs=in_specs, out_specs=out_specs, check_vma=False)
```

```python
import functools

import jax
import jax.numpy as jnp
from jax import lax
from jax.experimental import pallas as pl
from jax.experimental.pallas import tpu as pltpu
from jax.sharding import PartitionSpec as P

first_beta = 0.9
second_beta = 0.99
decay_rate = 0.1
learn_rate = 0.001
soft_width = 0.05

WIDTH = 256
LAGS = (2, 10, 16, 20, 23)
SLOTS = 3
HELD = LAGS[-1] + 1
MESH = pl.DeviceIdType.MESH


def block_product(columns, dout):
    dims = (((0,), (0,)), ((), ()))
    return lax.dot_general(columns, dout, dims, preferred_element_type=jnp.float32)


def mask_tokens(hidden, counts, bucket_expert):
    catalog = lax.broadcasted_iota(jnp.int32, counts.shape, 1)
    own_count = jnp.sum(jnp.where(catalog == bucket_expert[0], counts, 0))
    position = lax.broadcasted_iota(jnp.int32, (hidden.shape[0], 1), 0)
    return own_count, jnp.where(position < own_count, hidden, jnp.zeros_like(hidden))


def lion(grad, param, momentum):
    blend = first_beta * momentum + (1.0 - first_beta) * grad
    direction = jnp.tanh(blend / soft_width) + decay_rate * param
    new_param = param - learn_rate * direction
    new_momentum = second_beta * momentum + (1.0 - second_beta) * grad
    return (new_param, new_momentum, direction)


def plain_body(hidden, dout, counts, bucket_expert, param, momentum):
    own_count, masked = mask_tokens(hidden, counts, bucket_expert)
    total = lax.psum(own_count, ("dp", "expert")).astype(jnp.float32)
    shard = lax.psum_scatter(
        block_product(masked, dout), ("dp", "expert"), scatter_dimension=0, tiled=True
    )
    return lion(shard / total, param, momentum)


def reduce_kernel(
    chunks, ht_ref, dout_ref, count_ref, shard_ref, total_ref,
    acc, r0, r1, r2, r3, r4, tiles, count_in,
    tile_sem, send_sem, recv_sem, count_send, count_recv,
):
    rows = acc.shape[2]
    landing = (r0, r1, r2, r3, r4)
    dp = lax.axis_index("dp")
    ex = lax.axis_index("expert")
    y, x = lax.div(dp, 2), lax.rem(dp, 2)
    z1, z0, core = lax.div(ex, 4), lax.rem(lax.div(ex, 2), 2), lax.rem(ex, 2)
    step_x, step_y = 1 - 2 * x, 2 - 4 * y
    step_core, step_z0, step_z1 = 1 - 2 * core, 2 - 4 * z0, 4 - 8 * z1
    partners = (
        (dp, ex + step_core), (dp + step_x, ex), (dp + step_y, ex),
        (dp, ex + step_z0), (dp, ex + step_z1),
    )

    def tile_copy(c):
        slot = lax.rem(c, SLOTS)
        columns = pl.ds(pl.multiple_of(c * WIDTH, WIDTH), WIDTH)
        return pltpu.make_async_copy(
            dout_ref.at[:, columns], tiles.at[slot], tile_sem.at[slot]
        )

    def kind(c):
        z_first = lax.div(lax.rem(c, 9), 7)
        return z_first, lax.rem(c, 2)

    def exchange(c, stage):
        half = landing[stage].shape[1]
        if stage == 0:
            target = (dp, ex + step_core)
        else:
            z_first, parity = kind(c)
            on_dp = z_first if stage >= 3 else 1 - z_first
            swap = parity if stage in (1, 3) else 1 - parity
            step_dp = (1 - swap) * step_x + swap * step_y
            step_ex = step_z0 if stage in (1, 3) else step_z1
            target = (dp + on_dp * step_dp, ex + (1 - on_dp) * step_ex)
        return pltpu.make_async_remote_copy(
            src_ref=acc.at[lax.rem(c, HELD), pl.ds(half, half)],
            dst_ref=landing[stage].at[c],
            send_sem=send_sem.at[stage, c],
            recv_sem=recv_sem.at[stage, c],
            device_id=target,
            device_id_type=MESH,
        )

    def count_exchange(stage):
        return pltpu.make_async_remote_copy(
            src_ref=count_in.at[stage],
            dst_ref=count_in.at[5 + stage],
            send_sem=count_send.at[stage],
            recv_sem=count_recv.at[stage],
            device_id=partners[stage],
            device_id_type=MESH,
        )

    for c in range(SLOTS):
        tile_copy(c).start()
    barrier = pltpu.get_barrier_semaphore()
    for partner in partners:
        pl.semaphore_signal(barrier, inc=1, device_id=partner, device_id_type=MESH)
    pl.semaphore_wait(barrier, 5)
    count_in[0] = count_ref[...]
    count_exchange(0).start()

    def multiply(c):
        tile_copy(c).wait()
        z_first, parity = kind(c)
        w_first, w_second = 8 - 6 * z_first, 4 - 3 * z_first
        w_x = (1 - parity) * w_first + parity * w_second
        w_y = parity * w_first + (1 - parity) * w_second
        w_z0, w_z1 = 2 + 6 * z_first, 1 + 3 * z_first
        mine = (y, x, z1, z0, core)
        weights = (w_y, w_x, w_z1, w_z0, 16)
        off = [
            [bit * weight for bit, weight in zip(mine, weights)],
            [(1 - bit) * weight for bit, weight in zip(mine, weights)],
        ]
        product = jnp.dot(
            ht_ref[...], tiles[lax.rem(c, SLOTS)], preferred_element_type=jnp.float32
        )
        held = lax.rem(c, HELD)
        for block in range(2 ** len(mine)):
            place = 0
            for i in range(len(mine)):
                place = place + off[(block >> (len(mine) - 1 - i)) & 1][i]
            acc[held, place] = product[block * rows:(block + 1) * rows]
        exchange(c, 0).start()

        @pl.when(c + SLOTS < chunks)
        def _():
            tile_copy(c + SLOTS).start()

    def fold(c, stage):
        half = landing[stage].shape[1]
        exchange(c, stage).wait_recv()
        held = lax.rem(c, HELD)
        acc[held, 0:half] = acc[held, 0:half] + landing[stage][c]
        exchange(c, stage + 1).start()

    def finish(c):
        exchange(c, 4).wait_recv()
        columns = pl.ds(pl.multiple_of(c * WIDTH, WIDTH), WIDTH)
        shard_ref[:, columns] = acc[lax.rem(c, HELD), 0] + r4[c, 0]
        for stage in range(5):
            exchange(c, stage).wait_send()

    def step(k, carry):
        @pl.when(k < chunks)
        def _():
            multiply(k)

        for stage in range(4):
            c = k - LAGS[stage]

            @pl.when((c >= 0) & (c < chunks))
            def _():
                fold(c, stage)

        c = k - LAGS[4]

        @pl.when(c >= 0)
        def _():
            finish(c)

        for stage in range(4):
            @pl.when(k == 3 * stage + 3)
            def _():
                count_exchange(stage).wait_recv()
                count_in[stage + 1] = count_in[stage] + count_in[5 + stage]
                count_exchange(stage + 1).start()

        return carry

    lax.fori_loop(0, chunks + LAGS[4], step, 0)
    count_exchange(4).wait_recv()
    total_ref[...] = count_in[4] + count_in[9]

    for stage in range(5):
        count_exchange(stage).wait_send()


def fast_body(devices, hidden, dout, counts, bucket_expert, param, momentum):
    own_count, masked = mask_tokens(hidden, counts, bucket_expert)
    tokens, features = hidden.shape
    width = dout.shape[1]
    rows = features // devices
    chunks = width // WIDTH
    spread = jnp.full((8, 128), own_count.astype(jnp.float32))
    vmem = pl.BlockSpec(memory_space=pltpu.VMEM)
    shard, total = pl.pallas_call(
        functools.partial(reduce_kernel, chunks),
        out_shape=(
            jax.ShapeDtypeStruct((rows, width), jnp.float32),
            jax.ShapeDtypeStruct((8, 128), jnp.float32),
        ),
        in_specs=[vmem, pl.BlockSpec(memory_space=pl.ANY), vmem],
        out_specs=(vmem, vmem),
        scratch_shapes=[pltpu.VMEM((HELD, devices, rows, WIDTH), jnp.float32)]
        + [
            pltpu.VMEM((chunks, devices >> (s + 1), rows, WIDTH), jnp.float32)
            for s in range(5)
        ]
        + [
            pltpu.VMEM((SLOTS, tokens, WIDTH), jnp.bfloat16),
            pltpu.VMEM((10, 8, 128), jnp.float32),
            pltpu.SemaphoreType.DMA((SLOTS,)),
            pltpu.SemaphoreType.DMA((5, chunks)),
            pltpu.SemaphoreType.DMA((5, chunks)),
            pltpu.SemaphoreType.DMA((5,)),
            pltpu.SemaphoreType.DMA((5,)),
        ],
        compiler_params=pltpu.CompilerParams(
            collective_id=0, has_side_effects=True, vmem_limit_bytes=67043328
        ),
    )(masked.T, dout, spread)
    return lion(shard / total[0, 0], param, momentum)


def solution(mesh):
    spec = P(("dp", "expert"), None)
    in_specs = (spec, spec, spec, P(), spec, spec)
    out_specs = (spec, spec, spec)
    if mesh.shape["dp"] == 4 and mesh.shape["expert"] == 8:
        body = functools.partial(fast_body, mesh.size)
    else:
        body = plain_body
    return jax.shard_map(body, mesh=mesh, in_specs=in_specs, out_specs=out_specs, check_vma=False)
```
